64 devices in a mesh: dp: 4 (over x, y), tp: 16 (over z, core).
Axes of the slice: x: 2, y: 2, z: 8, core: 2. Of those that a mesh axis runs over, the one named last changes fastest.
The devices are a block of a 4x4x8 slice.
Arguments:
- query: bfloat16 [32, 32, 128], P('dp', 'tp'), parts along dimension 0
- k_cache: bfloat16 [32, 2048, 16, 128], P('dp', None, 'tp'), parts along dimension 0
- v_cache: bfloat16 [32, 2048, 16, 128], P('dp', None, 'tp'), parts along dimension 0
- k_new: bfloat16 [32, 16, 128], P('dp', 'tp'), parts along dimension 0
- v_new: bfloat16 [32, 16, 128], P('dp', 'tp'), parts along dimension 0
- lens: int32 [32], P('dp'), parts along dimension 0
Outputs:
- output 1: bfloat16 [32, 32, 128], P('dp', 'tp'), parts along dimension 0
- output 2: bfloat16 [32, 2048, 16, 128], P('dp', 'tp'), parts along dimension 0
- output 3: bfloat16 [32, 2048, 16, 128], P('dp', 'tp'), parts along dimension 0
There are 4 independent parts. The reference program is written for one: setup_inputs(seed, part) draws one part's arguments, and reference() takes and returns one part's arrays. A program takes and returns all parts, laid end to end along the dimension named above; each array names one.
All inputs are finite; a program needn't handle non-finite values.
Results may differ from the reference program's by a relative error of at most 0.00785484.
Values are sent between devices in bfloat16 or wider.
A program may use at most 768 MiB of HBM per device.

```python
import math
import jax
import jax.numpy as jnp
from jax import lax

BATCH = 8
SEQ_LEN = 2048
Q_HEADS = 32
KV_HEADS = 16
HEAD_DIM = 128


def setup_inputs(seed: int = 0, part: int = 0) -> dict:
    base_key = jax.random.fold_in(jax.random.key(seed), part)
    keys = jax.random.split(base_key, 6)
    group_size = Q_HEADS // KV_HEADS
    spread = math.sqrt(math.log(SEQ_LEN))
    align = 1.4 * math.sqrt(math.log(SEQ_LEN) / HEAD_DIM)
    cache_shape = (BATCH, SEQ_LEN, KV_HEADS, HEAD_DIM)
    k_cache = jax.random.normal(keys[0], cache_shape, jnp.float32)
    v_cache = jax.random.normal(keys[1], cache_shape, jnp.float32)
    k_new = jax.random.normal(keys[2], (BATCH, KV_HEADS, HEAD_DIM), jnp.float32)
    v_new = jax.random.normal(keys[3], (BATCH, KV_HEADS, HEAD_DIM), jnp.float32)
    noise = jax.random.normal(keys[4], (BATCH, KV_HEADS, group_size, HEAD_DIM), jnp.float32)
    mixed = math.sqrt(1.0 - align * align) * noise + align * k_new[:, :, None, :]
    query = (spread * mixed).reshape(BATCH, Q_HEADS, HEAD_DIM)
    len_keys = jax.random.split(keys[5])
    low_len = SEQ_LEN // 8
    lens = jax.random.randint(len_keys[0], (BATCH,), low_len, SEQ_LEN, jnp.int32)
    top_slot = jax.random.randint(len_keys[1], (), 0, BATCH, jnp.int32)
    lens = jnp.where(jnp.arange(BATCH) == top_slot, SEQ_LEN - 1, lens)
    return {"query": query.astype(jnp.bfloat16), "k_cache": k_cache.astype(jnp.bfloat16), "v_cache": v_cache.astype(jnp.bfloat16), "k_new": k_new.astype(jnp.bfloat16), "v_new": v_new.astype(jnp.bfloat16), "lens": lens}


def reference(query, k_cache, v_cache, k_new, v_new, lens):
    positions = jnp.arange(SEQ_LEN, dtype=jnp.int32)
    new_slot = (positions[None, :] == lens[:, None])[:, :, None, None]
    k_upd = jnp.where(new_slot, k_new[:, None], k_cache)
    v_upd = jnp.where(new_slot, v_new[:, None], v_cache)
    group_size = Q_HEADS // KV_HEADS
    inv_sqrt = HEAD_DIM ** -0.5

    def one_head(head_in):
        q_head, k_head, v_head, length = head_in
        scores = jnp.dot(q_head, k_head.T, preferred_element_type=jnp.float32) * inv_sqrt
        scores = jnp.where(positions[None, :] <= length, scores, -1e30)
        probs = jax.nn.softmax(scores, axis=-1)
        return jnp.dot(probs.astype(jnp.bfloat16), v_head, preferred_element_type=jnp.float32)

    q_flat = query.reshape(BATCH * KV_HEADS, group_size, HEAD_DIM)
    k_flat = jnp.swapaxes(k_upd, 1, 2).reshape(BATCH * KV_HEADS, SEQ_LEN, HEAD_DIM)
    v_flat = jnp.swapaxes(v_upd, 1, 2).reshape(BATCH * KV_HEADS, SEQ_LEN, HEAD_DIM)
    len_flat = jnp.repeat(lens, KV_HEADS)
    head_out = lax.map(one_head, (q_flat, k_flat, v_flat, len_flat))
    attn_out = head_out.reshape(BATCH, Q_HEADS, HEAD_DIM).astype(jnp.bfloat16)
    return attn_out, k_upd, v_upd
```

```python
import jax
import jax.numpy as jnp
from jax import lax
from jax.experimental import pallas as pl
from jax.experimental.pallas import tpu as pltpu
from jax.sharding import PartitionSpec as P

MASK_VALUE = -1e30
MESH = pl.DeviceIdType.MESH


def exchange_kernel(n, q_ref, k_hbm, v_hbm, kn_hbm, vn_hbm, kn_ref, vn_ref, lens_ref,
                    o_ref, rk, rv, rkn, rvn, kbuf, vbuf, load_sem, own_sem, send_sem, recv_sem):
    me = lax.axis_index("tp")
    batch, seq_len, head_dim = k_hbm.shape
    chunk = seq_len // n
    chips = n // 2
    chip, core = me // 2, me % 2

    loads = []
    for b in range(batch):
        for which, (src, dst) in enumerate(((k_hbm, kbuf), (v_hbm, vbuf))):
            loads.append(pltpu.make_async_copy(src.at[b], dst.at[b], load_sem.at[which, b]))
    for load in loads:
        load.start()

    barrier = pltpu.get_barrier_semaphore()
    for off in range(1, n):
        pl.semaphore_signal(barrier, inc=1, device_id={"tp": lax.rem(me + off, n)}, device_id_type=MESH)
    pl.semaphore_wait(barrier, n - 1)

    order = []
    for dist in range(chips // 2, 0, -1):
        steps = (dist,) if 2 * dist == chips else (dist, chips - dist)
        for step in steps:
            for other in (0, 1):
                order.append((step, other))
    order.append((0, 1))

    copies = []
    for step, other in order:
        peer = 2 * lax.rem(chip + step, chips) + lax.rem(core + other, 2)
        back = 2 * lax.rem(chip + chips - step, chips) + lax.rem(core + other, 2)
        window = pl.ds(pl.multiple_of(peer * chunk, chunk), chunk)
        for which, (src, dst) in enumerate(((kn_hbm, rkn), (vn_hbm, rvn))):
            copies.append((pltpu.make_async_remote_copy(
                src_ref=src, dst_ref=dst.at[me], send_sem=send_sem.at[2 + which, peer],
                recv_sem=recv_sem.at[2 + which, me], device_id={"tp": peer}, device_id_type=MESH),
                pltpu.make_async_copy(src, dst.at[back], recv_sem.at[2 + which, back])))
        for which, (src, dst) in enumerate(((k_hbm, rk), (v_hbm, rv))):
            copies.append((pltpu.make_async_remote_copy(
                src_ref=src.at[:, window], dst_ref=dst.at[me], send_sem=send_sem.at[which, peer],
                recv_sem=recv_sem.at[which, me], device_id={"tp": peer}, device_id_type=MESH),
                pltpu.make_async_copy(src.at[:, window], dst.at[back], recv_sem.at[which, back])))
    for copy, _ in copies:
        copy.start()

    for load in loads:
        load.wait()
    mine = pl.ds(pl.multiple_of(me * chunk, chunk), chunk)
    own = [pltpu.make_async_copy(kbuf.at[:, mine], rk.at[me], own_sem.at[0]),
           pltpu.make_async_copy(vbuf.at[:, mine], rv.at[me], own_sem.at[1]),
           pltpu.make_async_copy(kn_ref, rkn.at[me], own_sem.at[2]),
           pltpu.make_async_copy(vn_ref, rvn.at[me], own_sem.at[3])]
    for copy in own:
        copy.start()

    scale = head_dim ** -0.5

    def attend(b, carry):
        q = q_ref[b]
        length = lens_ref[b]
        row = lax.broadcasted_iota(jnp.int32, (batch, head_dim), 0) == b
        k_new = jnp.sum(jnp.where(row, kn_ref[...].astype(jnp.float32), 0.0), axis=0, keepdims=True)
        v_new = jnp.sum(jnp.where(row, vn_ref[...].astype(jnp.float32), 0.0), axis=0, keepdims=True)
        s = lax.dot_general(q, kbuf[b], (((1,), (1,)), ((), ())), preferred_element_type=jnp.float32)
        s_new = jnp.sum(q.astype(jnp.float32) * k_new, axis=1, keepdims=True)
        pos = lax.broadcasted_iota(jnp.int32, s.shape, 1)
        s = jnp.where(pos == length, s_new, s) * scale
        s = jnp.where(pos <= length, s, MASK_VALUE)
        e = jnp.exp(s - jnp.max(s, axis=1, keepdims=True))
        p = (e / jnp.sum(e, axis=1, keepdims=True)).astype(jnp.bfloat16).astype(jnp.float32)
        p_new = jnp.sum(jnp.where(pos == length, p, 0.0), axis=1, keepdims=True)
        p_old = jnp.where(pos == length, 0.0, p).astype(jnp.bfloat16)
        o = jnp.dot(p_old, vbuf[b], preferred_element_type=jnp.float32) + p_new * v_new
        o_ref[b] = o.astype(o_ref.dtype)
        return carry

    lax.fori_loop(0, batch, attend, 0)

    for copy in own:
        copy.wait()
    for copy, arrival in copies:
        copy.wait_send()
    for copy, arrival in copies:
        arrival.wait()


def solution(mesh):
    n = mesh.shape["tp"]

    def local_step(query, k_cache, v_cache, k_new, v_new, lens):
        batch, seq_len, _, head_dim = k_cache.shape
        chunk = seq_len // n
        k = k_cache.reshape(batch, seq_len, head_dim)
        v = v_cache.reshape(batch, seq_len, head_dim)
        kn = k_new.reshape(batch, head_dim)
        vn = v_new.reshape(batch, head_dim)
        anywhere = pl.BlockSpec(memory_space=pl.ANY)
        vmem = pl.BlockSpec(memory_space=pltpu.VMEM)
        dtype = k.dtype
        attn, rk, rv, rkn, rvn = pl.pallas_call(
            lambda *refs: exchange_kernel(n, *refs),
            name="exchange",
            out_shape=(jax.ShapeDtypeStruct(query.shape, query.dtype),
                       jax.ShapeDtypeStruct((n, batch, chunk, head_dim), dtype),
                       jax.ShapeDtypeStruct((n, batch, chunk, head_dim), dtype),
                       jax.ShapeDtypeStruct((n, batch, head_dim), dtype),
                       jax.ShapeDtypeStruct((n, batch, head_dim), dtype)),
            in_specs=[vmem, anywhere, anywhere, anywhere, anywhere, vmem, vmem,
                      pl.BlockSpec(memory_space=pltpu.SMEM)],
            out_specs=(vmem, anywhere, anywhere, anywhere, anywhere),
            scratch_shapes=[
                pltpu.VMEM((batch, seq_len, head_dim), dtype),
                pltpu.VMEM((batch, seq_len, head_dim), dtype),
                pltpu.SemaphoreType.DMA((2, batch)),
                pltpu.SemaphoreType.DMA((4,)),
                pltpu.SemaphoreType.DMA((4, n)),
                pltpu.SemaphoreType.DMA((4, n)),
            ],
            compiler_params=pltpu.CompilerParams(collective_id=0, has_side_effects=True),
        )(query, k, v, kn, vn, kn, vn, lens)

        pos = lax.axis_index("tp") * chunk + lax.broadcasted_iota(jnp.int32, (1, chunk, 1, 1), 1)
        new_slot = pos == lens[:, None, None, None]

        def finish(received, new):
            rows = jnp.transpose(received, (1, 2, 0, 3))
            return jnp.where(new_slot, jnp.transpose(new, (1, 0, 2))[:, None], rows)

        return attn, finish(rk, rkn), finish(rv, rvn)

    head_spec = P("dp", "tp")
    entry_spec = P("dp", None, "tp")
    return jax.shard_map(local_step, mesh=mesh, in_specs=(head_spec, entry_spec, entry_spec, head_spec, head_spec, P("dp")), out_specs=(head_spec, P("dp", "tp"), P("dp", "tp")), check_vma=False)
```
